32 devices in a mesh: parts: 2 (over x), seq: 8 (over z, y), tp: 2 (over core).
Axes of the slice: x: 2, y: 2, z: 4, core: 2. Of those that a mesh axis runs over, the one named last changes fastest.
Arguments:
- video_q: bfloat16 [4096, 1024], P(('parts', 'seq', 'tp')), parts along dimension 0, may hold values from -6 to 6
- video_k: bfloat16 [4096, 1024], P(('parts', 'seq', 'tp')), parts along dimension 0, may hold values from -6 to 6
- video_v: bfloat16 [4096, 1024], P(('parts', 'seq', 'tp')), parts along dimension 0, may hold values from -6 to 6
- cross_q: bfloat16 [4096, 1024], P(('parts', 'seq', 'tp')), parts along dimension 0, may hold values from -6 to 6
- qk_gains: float32 [4, 1024], replicated, may hold values from 1 to 2
- captions: bfloat16 [4096, 4096], P(('parts', 'seq'), 'tp'), parts along dimension 0, may hold values from -16 to 16
- text_gain: float32 [4096], P('tp'), may hold values from 0.25 to 1.75
- cross_kv_weight: bfloat16 [4096, 2, 1024], P('tp', None, 'seq'), may hold values from -0.09375 to 0.09375
- lengths: int32 [8], P('parts'), parts along dimension 0, may hold values from 1 to 512, 1024 in all
- video_prompt: int32 [8], P('parts'), parts along dimension 0, may hold values from 0 to 3, each once
Outputs:
- self_out: bfloat16 [4096, 1024], P(('parts', 'seq', 'tp')), parts along dimension 0
- cross_out: bfloat16 [4096, 1024], P(('parts', 'seq', 'tp')), parts along dimension 0
The draws below stay inside these ranges and needn't reach their ends.
There are 2 independent parts, one for each index of `parts`. The reference program is written for one: setup_inputs(seed, part) draws one part's arguments, and reference() takes and returns one part's arrays. A program takes and returns all parts, laid end to end along the dimension named above; an argument that names none is the same for every part. Nothing has to cross between parts.
Inputs may be any that keep to these rules, and one draw needn't show every extreme that they name: The lengths of a group's captions add up to 1024, and one caption has exactly 512. `video_prompt`: every caption belongs to exactly one video.
All inputs are finite; a program needn't handle non-finite values.
Results may differ from the reference program's by a relative error of at most 0.011.
Values may be sent and summed in bfloat16 or wider, within the bound.
No kernel may reach another device: no remote copies, remote signals or barrier semaphores. Data moves between devices by JAX's collectives and lax.ppermute only.
A program may use at most 128 MiB of HBM per device.

```python
import math
import jax
import jax.numpy as jnp
import numpy as np
from jax import lax

DT = 4096
HD = 128
HEADS = 8
DM = 1024
VIDEOS = 4
PROMPTS = 4
CAP = 512
CAP_VALID = 1024
TOKENS = 2048


def draw_captions(key, part):
    noise_key = jax.random.fold_in(key, 0)
    values = jax.random.normal(noise_key, (PROMPTS * CAP, DT), jnp.float32)
    return jnp.clip(values, -16.0, 16.0).astype(jnp.bfloat16)


def shard_levels(key, extent, shards, low, top_value):
    level, own = 1.0, jax.random.fold_in(key, 6)
    for position, shards_of in shards:
        draws = jnp.exp(jax.random.uniform(jax.random.fold_in(own, position), (shards_of,), jnp.float32, low / len(shards), top_value / len(shards)))
        level = level * jnp.repeat(draws, extent[position] // shards_of).reshape([-1 if axis == position else 1 for axis in range(len(extent))])
    return level


def profile(count, total, most, lean):
    loads = [(1 << 20) // math.isqrt(rank ** lean) + 1 for rank in range(2, count + 1)]
    spare, holding = total - most - (count - 1), [1] * (count - 1)
    while spare > 0:
        candidates = [i for i in range(count - 1) if holding[i] < most]
        mass, left = sum([loads[i] for i in candidates]), spare
        for i in candidates:
            extra = min(most - holding[i], max(1, left * loads[i] // mass), spare)
            holding[i] = holding[i] + extra
            spare = spare - extra
    return np.array([most] + holding)


def ragged(own_key, number_of, total, most, lean):
    if number_of == 2:
        one = jax.random.randint(own_key, (), max(1, total - most), min(most, total - 1) + 1)
        return jnp.stack([one, total - one])
    tallies = jnp.asarray(profile(number_of, total, most, lean), jnp.int32)
    pairs = (number_of - 1) // 2
    giver, receiver = tallies[1:1 + 2 * pairs:2], tallies[2:2 + 2 * pairs:2]
    margin = jnp.minimum(giver - 1, most - receiver)
    shifted = jax.random.randint(jax.random.fold_in(own_key, 1), (pairs,), 0, 1 << 20) % (margin + 1)
    tallies = tallies.at[1:1 + 2 * pairs:2].set(giver - shifted).at[2:2 + 2 * pairs:2].set(receiver + shifted)
    return tallies[jax.random.permutation(jax.random.fold_in(own_key, 2), number_of)]


def bell_draw(own_key, dims, scale, bound, cuts=(), kind=jnp.bfloat16):
    result = scale * jax.random.normal(own_key, dims, jnp.float32)
    if cuts:
        result = result * shard_levels(own_key, dims, cuts, -0.22, 0.18)
    return jnp.clip(result, -bound, bound).astype(kind)


def setup_inputs(seed: int = 0, part: int = 0) -> dict:
    seeds = jax.random.split(jax.random.key(seed), 11)
    own_keys = jax.random.split(jax.random.fold_in(seeds[10], part), 11)
    video_q = bell_draw(own_keys[0], (TOKENS, DM), 1.0, 6.0, ((0, 16),))
    video_k = bell_draw(own_keys[1], (TOKENS, DM), 1.0, 6.0, ((0, 16),))
    video_v = bell_draw(own_keys[2], (TOKENS, DM), 1.0, 6.0, ((0, 16),))
    cross_q = bell_draw(own_keys[3], (TOKENS, DM), 1.0, 6.0, ((0, 16),))
    qk_gains = jnp.clip(jnp.exp(jax.random.uniform(seeds[4], (4, DM), jnp.float32, math.log(1.0), math.log(2.0))), 1.0, 2.0)
    captions = draw_captions(jax.random.fold_in(jax.random.fold_in(seeds[10], part), 71), part)
    text_gain = jnp.clip(1.0 + 0.15 * jax.random.normal(seeds[6], (DT,), jnp.float32), 0.25, 1.75)
    cross_kv_weight = bell_draw(seeds[7], (DT, 2, DM), DT ** -0.5, 0.09375, ((0, 2), (2, 8)))
    lengths = ragged(own_keys[8], PROMPTS, CAP_VALID, CAP, 2).astype(jnp.int32)
    video_prompt = jax.random.permutation(own_keys[9], PROMPTS).astype(jnp.int32)
    return {"video_q": video_q, "video_k": video_k, "video_v": video_v, "cross_q": cross_q, "qk_gains": qk_gains, "captions": captions, "text_gain": text_gain, "cross_kv_weight": cross_kv_weight, "lengths": lengths, "video_prompt": video_prompt}


EPS = 1e-06

def head_norm(values, gain):
    inverse = lax.rsqrt(lax.optimization_barrier(jnp.mean(values * values, axis=-1, keepdims=True)) + EPS)
    return values * inverse * gain

def reference(video_q, video_k, video_v, cross_q, qk_gains, captions, text_gain, cross_kv_weight, lengths, video_prompt):
    text_rows = captions.astype(jnp.float32)
    inverse = lax.rsqrt(lax.optimization_barrier(jnp.mean(text_rows * text_rows, axis=1, keepdims=True)) + EPS)
    text_normed = (text_rows * inverse * text_gain[None, :]).astype(jnp.bfloat16)
    weight = cross_kv_weight.reshape(DT, 2 * HEADS * HD)
    key_value = jnp.dot(text_normed, weight, preferred_element_type=jnp.float32).reshape(PROMPTS, CAP, 2, HEADS, HD)
    head_gains = qk_gains.astype(jnp.float32).reshape(4, HEADS, HD)
    cross_keys = head_norm(key_value[:, :, 0], head_gains[3]).astype(jnp.bfloat16)
    cross_values = key_value[:, :, 1].astype(jnp.bfloat16)
    chosen_keys = jnp.transpose(cross_keys[video_prompt], (2, 0, 1, 3))
    chosen_values = jnp.transpose(cross_values[video_prompt], (2, 0, 1, 3))
    visible = jnp.arange(CAP, dtype=jnp.int32)[None, :] < lengths[video_prompt][:, None]

    def prepare(rows, gain):
        shaped = rows.astype(jnp.float32).reshape(TOKENS, HEADS, HD)
        return jnp.transpose(head_norm(shaped, gain).astype(jnp.bfloat16), (1, 0, 2))
    self_queries = prepare(video_q, head_gains[0])
    self_keys = prepare(video_k, head_gains[1])
    cross_queries = prepare(cross_q, head_gains[2])
    head_values = jnp.transpose(video_v.reshape(TOKENS, HEADS, HD), (1, 0, 2))
    score_scale = 1.0 / math.sqrt(HD)
    video_len = TOKENS // VIDEOS

    def one_head(operands):
        queries, key_rows, value_rows, cross_rows, cap_keys, cap_values = operands
        queries = queries.reshape(VIDEOS, video_len, HD).astype(jnp.float32)
        key_rows = key_rows.reshape(VIDEOS, video_len, HD).astype(jnp.float32)
        value_rows = value_rows.reshape(VIDEOS, video_len, HD).astype(jnp.float32)
        cross_rows = cross_rows.reshape(VIDEOS, video_len, HD).astype(jnp.float32)
        scores = jnp.einsum('vqd,vkd->vqk', queries, key_rows) * score_scale
        exp_scores = jnp.exp(scores)
        weights = (exp_scores / lax.optimization_barrier(jnp.sum(exp_scores, axis=2, keepdims=True))).astype(jnp.bfloat16)
        self_part = jnp.einsum('vqk,vkd->vqd', weights.astype(jnp.float32), value_rows).astype(jnp.bfloat16)
        cross_scores = jnp.einsum('vqd,vkd->vqk', cross_rows, cap_keys.astype(jnp.float32)) * score_scale
        cross_exp = jnp.where(visible[:, None, :], jnp.exp(cross_scores), 0.0)
        cross_weights = (cross_exp / lax.optimization_barrier(jnp.sum(cross_exp, axis=2, keepdims=True))).astype(jnp.bfloat16)
        cross_part = jnp.einsum('vqk,vkd->vqd', cross_weights.astype(jnp.float32), cap_values.astype(jnp.float32)).astype(jnp.bfloat16)
        return (self_part.reshape(TOKENS, HD), cross_part.reshape(TOKENS, HD))
    self_heads, cross_heads = lax.map(one_head, (self_queries, self_keys, head_values, cross_queries, chosen_keys, chosen_values))
    self_out = jnp.transpose(self_heads, (1, 0, 2)).reshape(TOKENS, HEADS * HD)
    cross_out = jnp.transpose(cross_heads, (1, 0, 2)).reshape(TOKENS, HEADS * HD)
    return (self_out, cross_out)
```

```python
import functools
import math

import jax
import jax.numpy as jnp
from jax import lax
from jax.experimental import pallas as pl
from jax.experimental.pallas import tpu as pltpu
from jax.sharding import PartitionSpec as P

EPS = 1e-06
AXES = ("parts", "seq", "tp")


def normed(values, gain):
    inverse = lax.rsqrt(jnp.mean(values * values, axis=-1, keepdims=True) + EPS)
    return (values * inverse * gain).astype(jnp.bfloat16)


def lookup(table, wanted):
    matches = wanted[..., None] == jnp.arange(table.shape[0], dtype=jnp.int32)
    return jnp.sum(jnp.where(matches, table, 0), axis=-1)


def self_kernel(q_ref, k_ref, v_ref, gq_ref, gk_ref, o_ref, *, scale):
    q = normed(q_ref[...].astype(jnp.float32), gq_ref[0])
    k = normed(k_ref[...].astype(jnp.float32), gk_ref[0])
    s = lax.dot_general(q, k, (((1,), (1,)), ((), ())), preferred_element_type=jnp.float32)
    e = jnp.exp(s * scale)
    total = jnp.sum(e, axis=1, keepdims=True)
    o = jnp.dot(e.astype(jnp.bfloat16), v_ref[...], preferred_element_type=jnp.float32)
    o_ref[...] = (o / total).astype(jnp.bfloat16)


def self_attention(q, k, v, gq, gk, heads, head_dim, scale):
    tokens = q.shape[0]
    spec = pl.BlockSpec((tokens, head_dim), lambda h: (0, h))
    gain_spec = pl.BlockSpec((1, 1, head_dim), lambda h: (h, 0, 0))
    return pl.pallas_call(
        functools.partial(self_kernel, scale=scale),
        grid=(heads,),
        in_specs=[spec, spec, spec, gain_spec, gain_spec],
        out_specs=spec,
        out_shape=jax.ShapeDtypeStruct(q.shape, jnp.bfloat16),
        name="self_attention",
    )(q, k, v, gq.reshape(heads, 1, head_dim), gk.reshape(heads, 1, head_dim))


def cross_kernel(info_ref, q_ref, k_ref, v_ref, gq_ref, o_ref, *, scale, members):
    slot = pl.program_id(0)
    length = info_ref[1, slot]
    member = info_ref[2, 0]
    q = normed(q_ref[0].astype(jnp.float32), gq_ref[0])
    total = None
    out = None
    for k in range(members):
        keys = k_ref[0, k]
        rows = keys.shape[0]
        s = lax.dot_general(q, keys, (((1,), (1,)), ((), ())), preferred_element_type=jnp.float32)
        first = lax.rem(member + k, members) * rows
        index = first + lax.broadcasted_iota(jnp.int32, s.shape, 1)
        e = jnp.where(index < length, jnp.exp(s * scale), 0.0)
        part = jnp.sum(e, axis=1, keepdims=True)
        o = jnp.dot(e.astype(jnp.bfloat16), v_ref[0, k], preferred_element_type=jnp.float32)
        total = part if total is None else total + part
        out = o if out is None else out + o
    o_ref[0] = (out / total).astype(jnp.bfloat16)


def cross_attention(q, keys, values, gain, info, scale):
    slots, tokens, head_dim = q.shape
    members, rows = keys.shape[1:3]
    spec = pl.BlockSpec((1, tokens, head_dim), lambda s, info: (s, 0, 0))
    kv_spec = pl.BlockSpec((1, members, rows, head_dim), lambda s, info: (info[0, s], 0, 0, 0))
    return pl.pallas_call(
        functools.partial(cross_kernel, scale=scale, members=members),
        grid_spec=pltpu.PrefetchScalarGridSpec(
            num_scalar_prefetch=1,
            grid=(slots,),
            in_specs=[spec, kv_spec, kv_spec, pl.BlockSpec((1, head_dim), lambda s, info: (0, 0))],
            out_specs=spec,
        ),
        out_shape=jax.ShapeDtypeStruct(q.shape, jnp.bfloat16),
        name="cross_attention",
    )(info, q, keys, values, gain.reshape(1, head_dim))


def make_per_device(mesh):
    parts_n, seq_n, tp_n = (mesh.shape[axis] for axis in AXES)

    def per_device(
        video_q,
        video_k,
        video_v,
        cross_q,
        qk_gains,
        captions,
        text_gain,
        cross_kv_weight,
        lengths,
        video_prompt,
    ):
        layers = video_prompt.shape[0]
        members = seq_n // layers
        half = layers // 2
        ranks = members * tp_n
        feats = captions.shape[1]
        head_dim = cross_kv_weight.shape[2]
        scale = 1.0 / math.sqrt(head_dim)
        assert half == tp_n and members * layers == seq_n
        part = lax.axis_index("parts")
        seq = lax.axis_index("seq")
        core = lax.axis_index("tp")
        layer = seq // members
        member = seq % members
        rank = member * tp_n + core
        lower = layer < half

        def permute(value, where):
            pairs = []
            for p in range(parts_n):
                for z in range(layers):
                    for m in range(members):
                        for t in range(tp_n):
                            target = where(p, z, m, t)
                            if target is None:
                                continue
                            q, y, n, u = target
                            pairs.append(
                                (
                                    (p * seq_n + z * members + m) * tp_n + t,
                                    (q * seq_n + y * members + n) * tp_n + u,
                                )
                            )
            return lax.ppermute(value, AXES, pairs)

        def to_middle(distance):
            def where(p, z, m, t):
                if z == half - 1 - distance:
                    return (p, half - 1, m, t)
                if z == half + distance:
                    return (p, half, m, t)
                return None

            return where

        def to_far_middle(distance):
            def where(p, z, m, t):
                if z == half - 1 - distance:
                    return (p, half, m, t)
                if z == half + distance:
                    return (p, half - 1, m, t)
                return None

            return where

        def from_middle(distance):
            def where(p, z, m, t):
                if z == half - 1:
                    return (p, half - 1 - distance, m, t)
                if z == half:
                    return (p, half + distance, m, t)
                return None

            return where

        def from_far_middle(distance):
            def where(p, z, m, t):
                if z == half - 1:
                    return (p, half + distance, m, t)
                if z == half:
                    return (p, half - 1 - distance, m, t)
                return None

            return where

        def turn_member(k):
            return lambda p, z, m, t: (p, z, (m + k) % members, t)

        def turn_part(k):
            return lambda p, z, m, t: ((p + k) % parts_n, z, m, t)

        def turn_core(k):
            return lambda p, z, m, t: (p, z, m, (t + k) % tp_n)

        def turn_rank(k):
            def where(p, z, m, t):
                r = (m * tp_n + t + k) % ranks
                return (p, z, r // tp_n, r % tp_n)

            return where

        def low_head(m, u):
            return (half - 1 - u) * members + m

        def high_head(m, u):
            return (half + u) * members + m

        def head_columns(rows, head):
            return lax.dynamic_slice_in_dim(rows, head * head_dim, head_dim, 1)

        near_rows = [captions]
        for d in range(1, half):
            near_rows.append(permute(captions, to_middle(d)))
        far_rows = [permute(rows, to_far_middle(0)) for rows in near_rows]
        slot_rows = near_rows + far_rows

        weight = cross_kv_weight.reshape(feats, 2 * head_dim)
        share = feats // parts_n
        weight_share = lax.dynamic_slice_in_dim(weight, part * share, share, 0)
        gain_column = text_gain[:, None]

        def whole_weight(piece):
            full = jnp.zeros((feats, 2 * head_dim), weight.dtype)
            full = lax.dynamic_update_slice_in_dim(full, piece, part * share, 0)
            for k in range(1, parts_n):
                other = permute(piece, turn_part(k))
                full = lax.dynamic_update_slice_in_dim(
                    full, other, ((part - k) % parts_n) * share, 0
                )
            return full

        columns = []
        for d in range(half):
            piece = weight_share if d == 0 else permute(weight_share, to_middle(d))
            for k in range(members):
                if k == 0 and d == 0:
                    full = weight
                elif k == 0:
                    full = whole_weight(piece)
                else:
                    full = whole_weight(permute(piece, turn_member(k)))
                scaled = full.astype(jnp.float32) * gain_column
                columns.append(scaled.astype(jnp.bfloat16))
        all_weight = jnp.concatenate(columns, axis=1)

        caption_values = captions.astype(jnp.float32)
        square_sums = jnp.sum(caption_values * caption_values, axis=1)
        square_sums = lax.psum(square_sums, "tp")
        inverse_own = lax.rsqrt(square_sums / (feats * tp_n) + EPS)
        inverse_all = lax.all_gather(inverse_own, "seq", axis=0, tiled=False)

        kept = None
        gathered = []
        for k in range(ranks):
            target = (rank + k) % ranks
            m, u = target // tp_n, target % tp_n
            low, high = low_head(m, u), high_head(m, u)
            block = jnp.concatenate(
                [
                    head_columns(rows, head)
                    for rows in (video_q, video_k, video_v, cross_q)
                    for head in (low, high)
                ],
                axis=1,
            )
            gathered.append(block if k == 0 else permute(block, turn_rank(k)))
        video_rows = jnp.concatenate(gathered, axis=0)
        wide = 2 * head_dim
        low, high = low_head(member, core), high_head(member, core)

        def gain_of(kind, head):
            return lax.dynamic_slice(qk_gains, (kind, head * head_dim), (1, head_dim))[0]

        self_rows = self_attention(
            video_rows[:, :wide],
            video_rows[:, wide : 2 * wide],
            video_rows[:, 2 * wide : 3 * wide],
            jnp.stack([gain_of(0, low), gain_of(0, high)]),
            jnp.stack([gain_of(1, low), gain_of(1, high)]),
            2,
            head_dim,
            scale,
        )

        cross_low = video_rows[:, 3 * wide : 3 * wide + head_dim]
        cross_high = video_rows[:, 3 * wide + head_dim :]
        cross_near = jnp.where(lower, cross_low, cross_high)
        cross_far = jnp.where(lower, cross_high, cross_low)
        near_queries = [cross_near]
        for d in range(1, half):
            near_queries.append(permute(cross_near, to_middle(d)))
        far_queries = [permute(cross_far, to_far_middle(d)) for d in range(half)]
        slot_queries = jnp.stack(near_queries + far_queries)

        steps = jnp.arange(half, dtype=jnp.int32)
        near_layers = jnp.where(lower, half - 1 - steps, half + steps)
        far_layers = jnp.where(lower, half + steps, half - 1 - steps)
        slot_layers = jnp.concatenate([near_layers, far_layers])
        owned_layer = jnp.where(lower, half - 1 - core, half + core)
        block_width = members * 2 * head_dim
        slot_keys, slot_values = [], []
        for s, rows in enumerate(slot_rows):
            product = jnp.dot(rows, all_weight, preferred_element_type=jnp.float32)
            key_value = lax.dynamic_slice_in_dim(product, core * block_width, block_width, 1)
            for k in range(1, tp_n):
                away = lax.dynamic_slice_in_dim(
                    product, ((core + k) % tp_n) * block_width, block_width, 1
                )
                key_value = key_value + permute(
                    away.astype(jnp.bfloat16), turn_core(k)
                ).astype(jnp.float32)
            inverse = lax.dynamic_index_in_dim(
                inverse_all, slot_layers[s] * members + member, 0, keepdims=False
            )
            key_value = key_value * inverse[:, None]
            key_parts, value_parts = [], []
            for k in range(members):
                head = owned_layer * members + (member - k) % members
                first = k * 2 * head_dim
                keys = normed(key_value[:, first : first + head_dim], gain_of(3, head))
                values = key_value[:, first + head_dim : first + 2 * head_dim].astype(jnp.bfloat16)
                both = jnp.concatenate([keys, values], axis=1)
                if k:
                    both = permute(both, turn_member(-k))
                key_parts.append(both[:, :head_dim])
                value_parts.append(both[:, head_dim:])
            slot_keys.append(jnp.stack(key_parts))
            slot_values.append(jnp.stack(value_parts))
        slot_keys = jnp.stack(slot_keys)
        slot_values = jnp.stack(slot_values)

        prompts = lookup(video_prompt, slot_layers)
        slot_lengths = lookup(lengths, prompts)
        slot_of = jnp.sum(
            jnp.where(
                prompts[:, None] == slot_layers[None, :],
                jnp.arange(layers, dtype=jnp.int32)[None, :],
                0,
            ),
            axis=1,
        )
        info = jnp.stack([slot_of, slot_lengths, jnp.broadcast_to(member, (layers,))])
        info = info.astype(jnp.int32)
        cross_out = cross_attention(
            slot_queries,
            slot_keys,
            slot_values,
            gain_of(2, owned_layer * members + member),
            info,
            scale,
        )

        distance = jnp.where(lower, half - 1 - layer, layer - half)
        near_out = cross_out[0]
        for d in range(1, half):
            near_out = jnp.where(distance == d, permute(cross_out[d], from_middle(d)), near_out)
        far_out = None
        for d in range(half):
            received = permute(cross_out[half + d], from_far_middle(d))
            far_out = received if d == 0 else jnp.where(distance == d, received, far_out)
        cross_rows = jnp.concatenate(
            [jnp.where(lower, near_out, far_out), jnp.where(lower, far_out, near_out)], axis=1
        )

        token_count = video_q.shape[0]

        def send_back(rows):
            result = jnp.zeros(video_q.shape, jnp.bfloat16)
            for k in range(ranks):
                block = rows[k * token_count : (k + 1) * token_count]
                if k:
                    block = permute(block, turn_rank(-k))
                source = (rank + k) % ranks
                m, u = source // tp_n, source % tp_n
                for column, head in ((0, low_head(m, u)), (1, high_head(m, u))):
                    piece = block[:, column * head_dim : (column + 1) * head_dim]
                    result = lax.dynamic_update_slice_in_dim(result, piece, head * head_dim, 1)
            return result

        return (send_back(self_rows), send_back(cross_rows))

    return per_device


def solution(mesh):
    return jax.shard_map(
        make_per_device(mesh),
        mesh=mesh,
        in_specs=(
            P(("parts", "seq", "tp"), None),
            P(("parts", "seq", "tp"), None),
            P(("parts", "seq", "tp"), None),
            P(("parts", "seq", "tp"), None),
            P(),
            P(("parts", "seq"), "tp"),
            P("tp"),
            P("tp", None, "seq"),
            P("parts"),
            P("parts"),
        ),
        out_specs=(P(("parts", "seq", "tp"), None), P(("parts", "seq", "tp"), None)),
        check_vma=False,
    )
```
